32 devices in a mesh: groups: 2 (over y), block: 4 (over z), seg: 2 (over x), sub: 2 (over core).
Axes of the slice: x: 2, y: 2, z: 4, core: 2. Of those that a mesh axis runs over, the one named last changes fastest.
Arguments:
- old_fields: float32 [2048, 4, 512], P(('groups', 'block', 'seg', 'sub')), parts along dimension 0, may hold values from -6 to 6
- corner_shift: float32 [24, 2048], P(None, ('groups', 'block', 'seg', 'sub')), parts along dimension 1, may hold values from -0.2 to 0.2
- targets: float32 [3, 131072], P(None, ('groups', 'block', 'seg', 'sub')), parts along dimension 1, may hold values from -0.7 to 0.7
- owners: int32 [1024], P(('groups', 'block', 'seg', 'sub')), parts along dimension 0, may hold values from 0 to 1023, as said below
Outputs:
- new_fields: float32 [4, 131072], P(None, ('groups', 'block', 'seg', 'sub')), parts along dimension 1
The draws below stay inside these ranges and needn't reach their ends.
There are 2 independent parts, one for each index of `groups`. The reference program is written for one: setup_inputs(seed, part) draws one part's arguments, and reference() takes and returns one part's arrays. A program takes and returns all parts, laid end to end along the dimension named above; each array names one. Nothing has to cross between parts.
Inputs may be any that keep to these rules, and one draw needn't show every extreme that they name: `owners`: owner e lies on device e // 64. At most 2 of the blocks on the rows of one device are owned by elements of any one device, and in every draw some device owns exactly 2 blocks of every device.
All inputs are finite; a program needn't handle non-finite values.
Results may differ from the reference program's by a relative error of at most 0.00029.
Values sent between devices are 32-bit elements; how exact they have to be, the bound alone decides.
A program may use at most 64 MiB of HBM per device.

```python
import jax
import jax.numpy as jnp
import numpy as np
from jax import lax

NVAR = 4
NODES = 512
NEWTON = 3
CAP = 2
BLK_DEV = 32
E_DEV = 64
ELEMS = 1024
POINTS = 65536


def draw_owners(key, part):
    device_count = ELEMS // E_DEV
    subkeys = jax.random.split(jax.random.fold_in(key, 7), 4)
    popular = jax.random.randint(subkeys[0], (), 0, device_count)
    others = jax.vmap(lambda sub_key: jax.random.permutation(sub_key, device_count - 1))(jax.random.split(subkeys[1], device_count))
    shuffle = jax.vmap(lambda sub_key: jax.random.permutation(sub_key, BLK_DEV))(jax.random.split(subkeys[2], device_count))
    position = jnp.arange(BLK_DEV, dtype=jnp.int32)
    spread_pick = others[:, (position - CAP) % (device_count - 1)]
    spread_dev = (popular + 1 + spread_pick) % device_count
    owner_dev = jnp.where(position[None, :] < CAP, popular, spread_dev)
    owner_dev = jnp.take_along_axis(owner_dev, shuffle, axis=1)
    element = jax.random.randint(subkeys[3], (device_count, BLK_DEV), 0, E_DEV)
    return (owner_dev * E_DEV + element).reshape(-1).astype(jnp.int32)


def block_scale(stream_key, dims, shards, low, largest):
    def one(axis_at, parts):
        heights = jax.random.uniform(jax.random.fold_in(jax.random.fold_in(stream_key, 6), axis_at), (parts,), jnp.float32, low / len(shards), largest / len(shards))
        return jnp.repeat(jnp.exp(heights), dims[axis_at] // parts).reshape((-1,) + (1,) * (len(dims) - axis_at - 1))

    factor_of = one(*shards[0])
    for cut in shards[1:]:
        factor_of = factor_of * one(*cut)
    return factor_of


def noise(stream_key, dims, scale, limit, cuts=(), held_as=jnp.bfloat16):
    values = jax.random.normal(stream_key, dims, jnp.float32) * scale
    if len(cuts) > 0:
        values = block_scale(stream_key, dims, cuts, -0.22, 0.18) * values
    return jnp.clip(values, min=-limit, max=limit).astype(held_as)


def setup_inputs(seed: int = 0, part: int = 0) -> dict:
    streams_of = jax.random.split(jax.random.key(seed), 5)
    part_splits = jax.random.split(jax.random.fold_in(streams_of[4], part), 5)
    return {
        "old_fields": noise(part_splits[0], (ELEMS, NVAR, NODES), 1.0, 6.0, ((0, 16),), jnp.float32),
        "corner_shift": jnp.clip(jax.random.uniform(part_splits[1], (24, ELEMS), jnp.float32, -0.2, 0.2) * block_scale(part_splits[1], (24, ELEMS), ((1, 16),), -0.4, 0.0), -0.2, 0.2),
        "targets": jnp.clip(jax.random.uniform(part_splits[2], (3, POINTS), jnp.float32, -0.7, 0.7) * block_scale(part_splits[2], (3, POINTS), ((1, 16),), -0.4, 0.0), -0.7, 0.7),
        "owners": draw_owners(jax.random.fold_in(jax.random.fold_in(streams_of[4], part), 71), part),
    }


GLL_POINTS = (-1.0, -0.8717401485096066, -0.5917001814331423, -0.2092992179024789, 0.2092992179024789, 0.5917001814331423, 0.8717401485096066, 1.0)
EXACT = lax.Precision.HIGHEST


def lagrange_rows(coords):
    gll_nodes = jnp.array(GLL_POINTS, jnp.float32)
    offsets = coords[None, :] - gll_nodes[:, None]
    spacing = gll_nodes[:, None] - gll_nodes[None, :] + jnp.eye(8, dtype=jnp.float32)
    diag_mask = jnp.eye(8, dtype=bool)
    factors = jnp.where(diag_mask[:, :, None], 1.0, offsets[None, :, :] / spacing[:, :, None])
    return jnp.prod(factors, axis=1)


def corner_signs():
    bit_table = np.array([[(corner >> (2 - coord_dim)) & 1 for corner in range(8)] for coord_dim in range(3)], np.float32)
    return jnp.asarray(2.0 * bit_table - 1.0)


def outer_prod(first, second, third):
    return (first[:, None, None, :] * second[None, :, None, :] * third[None, None, :, :]).reshape(8, -1)


def trilinear(ref_pos):
    shape_list = []
    slope_list = []
    for coord_dim in range(3):
        coordinate = ref_pos[coord_dim]
        shape_list.append(jnp.stack([0.5 - 0.5 * coordinate, 0.5 + 0.5 * coordinate]))
        slope_list.append(jnp.stack([jnp.full_like(coordinate, -0.5), jnp.full_like(coordinate, 0.5)]))
    values = outer_prod(shape_list[0], shape_list[1], shape_list[2])
    slopes = [outer_prod(slope_list[0], shape_list[1], shape_list[2]),
              outer_prod(shape_list[0], slope_list[1], shape_list[2]),
              outer_prod(shape_list[0], shape_list[1], slope_list[2])]
    return values, slopes


def solve_three(matrix, rhs_rows):
    cofactors = []
    for row_id in range(3):
        keep_rows = [remain for remain in range(3) if remain != row_id]
        cof_row = []
        for col_id in range(3):
            keep_cols = [remain for remain in range(3) if remain != col_id]
            sign_factor = 1.0 if (row_id + col_id) % 2 == 0 else -1.0
            cof_row.append(sign_factor * (matrix[keep_rows[0]][keep_cols[0]] * matrix[keep_rows[1]][keep_cols[1]]
                                          - matrix[keep_rows[0]][keep_cols[1]] * matrix[keep_rows[1]][keep_cols[0]]))
        cofactors.append(cof_row)
    determinant = matrix[0][0] * cofactors[0][0] + matrix[0][1] * cofactors[0][1] + matrix[0][2] * cofactors[0][2]
    return [(cofactors[0][col_id] * rhs_rows[0] + cofactors[1][col_id] * rhs_rows[1] + cofactors[2][col_id] * rhs_rows[2]) / determinant for col_id in range(3)]


def invert_map(corners, target):
    ref_pos = jnp.zeros_like(target)
    for iteration in range(NEWTON):
        values, slopes = trilinear(ref_pos)
        mapped = jnp.dot(corners, values, precision=EXACT)
        columns = [jnp.dot(corners, slope_row, precision=EXACT) for slope_row in slopes]
        matrix = [[columns[col_id][row_id] for col_id in range(3)] for row_id in range(3)]
        misfit = mapped - target
        update = solve_three(matrix, [misfit[row_id] for row_id in range(3)])
        ref_pos = jnp.clip(ref_pos - jnp.stack(update), -1.2, 1.2)
    return ref_pos


def interpolate(element_field, corners, target):
    ref_pos = invert_map(corners, target)
    along_x = lagrange_rows(ref_pos[0])
    along_y = lagrange_rows(ref_pos[1])
    along_z = lagrange_rows(ref_pos[2])
    weights = (along_y[:, None, :] * along_z[None, :, :]).reshape(64, -1)
    var_count = element_field.shape[0]
    partial_sum = jnp.dot(element_field.reshape(var_count * 8, 64), weights, precision=EXACT)
    return jnp.sum(partial_sum.reshape(var_count, 8, -1) * along_x[None, :, :], axis=1)


def reference(old_fields, corner_shift, targets, owners):
    block_count = owners.shape[0]
    block_points = targets.reshape(3, block_count, -1).transpose(1, 0, 2)
    cube_signs = corner_signs()

    def per_block(inputs):
        owner_id, target = inputs
        corners = cube_signs + corner_shift[:, owner_id].reshape(3, 8)
        return interpolate(old_fields[owner_id], corners, target)

    result = lax.map(per_block, (owners, block_points), batch_size=64)
    return result.transpose(1, 0, 2).reshape(old_fields.shape[1], -1)
```

```python
import functools

import jax
import jax.numpy as jnp
from jax import lax
from jax.experimental import pallas as pl
from jax.experimental.pallas import tpu as pltpu
from jax.sharding import PartitionSpec as P

NEWTON = 3
CAP = 2
GROUP_PEERS = 8
AXES = ("block", "seg", "sub")

GLL_POINTS = (
    -1.0,
    -0.8717401485096066,
    -0.5917001814331423,
    -0.2092992179024789,
    0.2092992179024789,
    0.5917001814331423,
    0.8717401485096066,
    1.0,
)
WEIGHTS = []
for _n in range(8):
    _w = 1.0
    for _m in range(8):
        if _m != _n:
            _w /= GLL_POINTS[_n] - GLL_POINTS[_m]
    WEIGHTS.append(_w)

F32 = jnp.float32
BF16 = jnp.bfloat16
EXACT = lax.Precision.HIGHEST
NT = (((1,), (1,)), ((), ()))


def iota(shape, dim):
    return lax.broadcasted_iota(jnp.int32, shape, dim)


def flip(index, static):
    bit = 1
    while bit <= static:
        if static & bit:
            index = index + bit * (1 - 2 * ((index // bit) % 2))
        bit *= 2
    return index


def newton(coef, y):
    def update(xi, jac, misfit):
        m = jac
        cof = [
            [m[1][1] * m[2][2] - m[1][2] * m[2][1], m[1][2] * m[2][0] - m[1][0] * m[2][2], m[1][0] * m[2][1] - m[1][1] * m[2][0]],
            [m[0][2] * m[2][1] - m[0][1] * m[2][2], m[0][0] * m[2][2] - m[0][2] * m[2][0], m[0][1] * m[2][0] - m[0][0] * m[2][1]],
            [m[0][1] * m[1][2] - m[0][2] * m[1][1], m[0][2] * m[1][0] - m[0][0] * m[1][2], m[0][0] * m[1][1] - m[0][1] * m[1][0]],
        ]
        inv = 1.0 / (m[0][0] * cof[0][0] + m[0][1] * cof[0][1] + m[0][2] * cof[0][2])
        out = []
        for b in range(3):
            step = (cof[0][b] * misfit[0] + cof[1][b] * misfit[1] + cof[2][b] * misfit[2]) * inv
            new = -step if xi is None else xi[b] - step
            out.append(jnp.clip(new, -1.2, 1.2))
        return out

    xi = update(None, [[c[4], c[2], c[1]] for c in coef], [c[0] - t for c, t in zip(coef, y)])
    for _ in range(NEWTON - 1):
        u, v, w = xi
        uv, uw, vw = u * v, u * w, v * w
        jac, misfit = [], []
        for c, t in zip(coef, y):
            du = c[4] + c[6] * v + c[5] * w + c[7] * vw
            dv = c[2] + c[6] * u + c[3] * w + c[7] * uw
            dw = c[1] + c[5] * u + c[3] * v + c[7] * uv
            jac.append([du, dv, dw])
            misfit.append((c[0] - t) + u * du + v * (c[2] + c[3] * w) + w * c[1])
        xi = update(xi, jac, misfit)
    return xi


def lagrange(x):
    diff = [x - t for t in GLL_POINTS]
    pre = [None, diff[0]]
    for n in range(2, 8):
        pre.append(pre[-1] * diff[n - 1])
    suf = [None] * 8
    suf[6] = diff[7]
    for n in range(5, -1, -1):
        suf[n] = suf[n + 1] * diff[n + 1]
    out = []
    for n in range(8):
        value = suf[n] if n == 0 else pre[n] if n == 7 else pre[n] * suf[n]
        out.append(value * WEIGHTS[n])
    return out


def kernel(sizes, group_peers, owners_ref, targets_ref, shift_ref, fields_hbm, out_ref,
           fbuf, table, send, recv, res, ret, lag, idsend, idrecv, ids, slotv, slots,
           fsem, idsem, idsem2, slotsem, s0, r0, s1, r1, s2, r2):
    nb, ns, nc = sizes
    n = nb * ns * nc
    blocks = owners_ref.shape[1]
    elems = shift_ref.shape[1]
    pts = out_ref.shape[2]
    groups = n // group_peers
    lanes = idsend.shape[1]
    here = [lax.axis_index(a) for a in AXES]
    me = (here[0] * ns + here[1]) * nc + here[2]

    def peer(k):
        if isinstance(k, int):
            return {
                "block": flip(here[0], k // (ns * nc)),
                "seg": flip(here[1], (k // nc) % ns),
                "sub": flip(here[2], k % nc),
            }
        other = jnp.bitwise_xor(me, k)
        return {"block": other // (ns * nc), "seg": (other // nc) % ns, "sub": other % nc}

    def rows(k, count=1):
        start = 8 * k
        return pl.ds(start if isinstance(start, int) else pl.multiple_of(start, 8), 8 * count)

    def remote(src, dst, ssem, rsem, k, g):
        part = rows(k) if src is send else pl.ds(CAP * k, CAP)
        return pltpu.make_async_remote_copy(
            src_ref=src.at[part], dst_ref=dst.at[part],
            send_sem=ssem, recv_sem=rsem.at[g],
            device_id=peer(k), device_id_type=pl.DeviceIdType.MESH)

    fetch = pltpu.make_async_copy(fields_hbm, fbuf, fsem)
    fetch.start()
    barrier = pltpu.get_barrier_semaphore()
    unrolled = n <= 32

    def for_peers(first, last, body):
        if unrolled:
            for k in reversed(range(first, last)):
                body(k)
        else:
            lax.fori_loop(first, last, lambda k, c: (body(k), c)[1], 0)

    for_peers(1, n, lambda k: pl.semaphore_signal(
        barrier, inc=1, device_id=peer(k), device_id_type=pl.DeviceIdType.MESH))

    shift_bits = elems.bit_length() - 1
    own = owners_ref[...]
    owner_dev = jnp.right_shift(own, shift_bits)
    local = (own - owner_dev * elems).astype(F32)
    hit = (jnp.bitwise_xor(iota((n, blocks), 0), me) == owner_dev).astype(F32)
    earlier = (iota((blocks, blocks), 0) < iota((blocks, blocks), 1)).astype(F32)
    rank = jnp.dot(hit, earlier, preferred_element_type=F32)
    match = [jnp.where(rank == float(c), hit, 0.0) for c in range(CAP)]
    both = jnp.concatenate(match, axis=0)
    cat = jnp.concatenate([targets_ref[:, a, :] for a in range(3)], axis=1)
    packed = jnp.dot(both, cat, precision=EXACT, preferred_element_type=F32)
    elem_rows = lax.dot_general(both, jnp.broadcast_to(local, (pts, blocks)), NT, preferred_element_type=F32)
    for c in range(CAP):
        part = slice(c * n, (c + 1) * n)
        for a in range(3):
            send[pl.ds(4 * c + a, n, stride=8), :] = packed[part, a * pts:(a + 1) * pts]
        send[pl.ds(4 * c + 3, n, stride=8), :] = elem_rows[part]
        for a in range(3):
            recv[4 * c + a:4 * c + a + 1, :] = packed[c * n:c * n + 1, a * pts:(a + 1) * pts]
        recv[4 * c + 3:4 * c + 4, :] = elem_rows[c * n:c * n + 1]
    square = (blocks, blocks)
    diag = iota(square, 0) == iota(square, 1)
    own_rows = jnp.broadcast_to(own, square)
    own_col = jnp.sum(jnp.where(diag, own_rows, 0), axis=1, keepdims=True)
    dev_col = jnp.right_shift(own_col, shift_bits)
    dev_row = jnp.right_shift(own_rows, shift_bits)
    same = jnp.where(dev_col == dev_row, 1, 0)
    rank_row = jnp.sum(jnp.where(iota(square, 0) < iota(square, 1), same, 0), axis=0, keepdims=True)
    rank_col = jnp.sum(jnp.where(iota(square, 1) < iota(square, 0), same, 0), axis=1, keepdims=True)
    place = jnp.minimum(CAP * jnp.bitwise_xor(owner_dev, me) + rank_row, CAP * n - 1)
    place = jnp.concatenate([place, jnp.zeros((1, pts - blocks), jnp.int32)], axis=1)
    goes = iota((blocks, lanes), 1) == jnp.bitwise_xor(dev_col, me)
    elem_col = own_col - dev_col * elems
    for c in range(CAP):
        mine = jnp.where(goes, jnp.where(rank_col == c, elem_col, 0), 0)
        idsend[c:c + 1, :] = jnp.sum(mine, axis=0, keepdims=True)
    slotv[...] = place
    slot_copy = pltpu.make_async_copy(slotv, slots, slotsem)
    slot_copy.start()

    pl.semaphore_wait(barrier, n - 1)
    for_peers(1, n, lambda k: remote(send, recv, s1, r1, k, k // group_peers).start())
    for_peers(1, n, lambda k: pltpu.make_async_remote_copy(
        src_ref=idsend, dst_ref=idrecv.at[k], send_sem=s0, recv_sem=r0.at[k // group_peers],
        device_id=peer(k), device_id_type=pl.DeviceIdType.MESH).start())

    row, col = iota((24, 24), 0), iota((24, 24), 1)
    both_bits = jnp.bitwise_and(row, col) % 8
    odd = (both_bits + both_bits // 2 + both_bits // 4) % 2
    hada = jnp.where(row // 8 == col // 8, (1 - 2 * odd).astype(F32) * 0.125, 0.0)
    bits = row % 8
    sign = (1 - 2 * ((bits + bits // 2 + bits // 4) % 2)).astype(F32)
    coefs = jnp.dot(hada * sign, shift_ref[...], precision=EXACT, preferred_element_type=F32)
    c_hi = coefs.astype(BF16)
    rest = coefs - c_hi.astype(F32)
    c_mid = rest.astype(BF16)
    c_lo = (rest - c_mid.astype(F32)).astype(BF16)

    fetch.wait()
    low_sub = iota((8, 128), 0) < 4
    low_lane = iota((8, 128), 1) < 64
    keep = low_sub == low_lane

    def split(e, carry):
        parts = []
        for q in range(4):
            x = fbuf[e, :, q * 128:(q + 1) * 128]
            x = jnp.concatenate([x, x], axis=0)
            hi = x.astype(BF16).astype(F32)
            lo = x - hi
            a = jnp.where(low_sub, hi, lo)
            b = pltpu.roll(jnp.where(low_sub, lo, hi), 64, axis=1)
            parts.append(jnp.where(keep, a, b))
        table[e] = jnp.concatenate(parts, axis=0).astype(BF16)
        return carry

    lax.fori_loop(0, elems, split, 0, unroll=4)

    per = group_peers
    count = CAP * per

    def run_group(g, first):
        base = g * per
        got = per - 1 if first else per
        start = base + 1 if first else base
        pltpu.make_async_copy(recv.at[rows(start, got), :], recv.at[rows(start, got), :], r1.at[g]).wait()

        def gather(a):
            return jnp.concatenate(
                [recv[pl.ds(8 * base + 4 * c + a, per, stride=8), :] for c in range(CAP)], axis=0)

        y = [gather(a) for a in range(3)]
        elem = gather(3)
        lane = iota((count, pts), 1)
        if first:
            own_ids = pltpu.make_async_copy(idsend, ids.at[0], idsem)
            own_ids.start()
        taken = idrecv.at[pl.ds(start, got)]
        pltpu.make_async_copy(taken, taken, r0.at[g]).wait()
        id_copy = pltpu.make_async_copy(taken, ids.at[pl.ds(start, got)], idsem2)
        id_copy.start()
        pick = jnp.where(elem[:, :elems] == lane[:, :elems].astype(F32), 1.0, 0.0).astype(BF16)
        chosen = sum(lax.dot_general(pick, c, NT, preferred_element_type=F32) for c in (c_hi, c_mid, c_lo))
        coef = []
        for a in range(3):
            line = []
            for m in range(8):
                value = chosen[:, 8 * a + m:8 * a + m + 1]
                if m == 4 >> a:
                    value = value + 1.0
                line.append(jnp.broadcast_to(value, (count, pts)))
            coef.append(line)
        xi = newton(coef, y)
        for a in range(3):
            for i, value in enumerate(lagrange(xi[a])):
                lag[a, pl.ds(i, count, stride=8), :] = value
        if first:
            own_ids.wait()
        id_copy.wait()
        for s in range(count):
            c, p = s // per, s % per
            e = ids[base + p, c, base + p]
            left = table[e]
            lz = lag[2, 8 * s:8 * s + 8, :]
            w = jnp.concatenate([lag[1, 8 * s + j:8 * s + j + 1, :] * lz for j in range(8)], axis=0)
            w_hi = w.astype(BF16)
            w_lo = (w - w_hi.astype(F32)).astype(BF16)
            prod = jnp.dot(
                jnp.concatenate([left, left], axis=1),
                jnp.concatenate([w_hi, w_hi, w_lo, w_lo], axis=0),
                preferred_element_type=F32)
            total = None
            for q in range(4):
                lx = jnp.where(low_sub, lag[0, 8 * s + 2 * q:8 * s + 2 * q + 1, :],
                               lag[0, 8 * s + 2 * q + 1:8 * s + 2 * q + 2, :])
                term = prod[8 * q:8 * q + 8] * lx
                total = term if total is None else total + term
            total = total[0:4] + total[4:8]
            if first and p == 0:
                ret[c] = total
            else:
                res[CAP * (base + p) + c] = total
        for_peers_in = range(1 if first else 0, per)
        for p in for_peers_in:
            remote(res, ret, s2, r2, base + p, g).start()

    run_group(0, True)
    if unrolled:
        for g in range(1, groups):
            run_group(g, False)
    else:
        lax.fori_loop(1, groups, lambda g, c: (run_group(g, False), c)[1], 0)

    slot_copy.wait()
    rest_rows = rows(1, n - 1)
    for g in range(groups):
        start, got = (1, per - 1) if g == 0 else (g * per, per)
        back = ret.at[pl.ds(CAP * start, CAP * got)]
        pltpu.make_async_copy(back, back, r2.at[g]).wait()
    for b in range(blocks):
        out_ref[b] = ret[slots[0, b]]
    pltpu.make_async_copy(idrecv.at[pl.ds(1, n - 1)], idrecv.at[pl.ds(1, n - 1)], s0).wait()
    pltpu.make_async_copy(send.at[rest_rows, :], send.at[rest_rows, :], s1).wait()
    left = res.at[pl.ds(CAP, CAP * (n - 1))]
    pltpu.make_async_copy(left, left, s2).wait()


def shards(sizes, old_fields, corner_shift, targets, owners):
    n = sizes[0] * sizes[1] * sizes[2]
    elems, nvar, nodes = old_fields.shape
    blocks = owners.shape[0]
    pts = targets.shape[1] // blocks
    assert n & (n - 1) == 0 and elems & (elems - 1) == 0 and nvar == 4 and nodes == 512
    group_peers = min(GROUP_PEERS, n)
    groups = n // group_peers
    lanes = 128 * ((n + 127) // 128)
    points = targets.reshape(3, blocks, pts).transpose(1, 0, 2)
    vmem = pl.BlockSpec(memory_space=pltpu.VMEM)
    message = pltpu.VMEM((8 * n, pts), F32)
    result = pltpu.VMEM((CAP * n, nvar, pts), F32)
    out = pl.pallas_call(
        functools.partial(kernel, sizes, group_peers),
        out_shape=jax.ShapeDtypeStruct((blocks, nvar, pts), F32),
        in_specs=[vmem, vmem, vmem, pl.BlockSpec(memory_space=pl.ANY)],
        out_specs=vmem,
        scratch_shapes=[
            pltpu.VMEM((elems, nvar, nodes), F32),
            pltpu.VMEM((elems, 32, 128), BF16),
            message, message, result, result,
            pltpu.VMEM((3, 8 * CAP * group_peers, pts), F32),
            pltpu.VMEM((CAP, lanes), jnp.int32),
            pltpu.VMEM((n, CAP, lanes), jnp.int32),
            pltpu.SMEM((n, CAP, lanes), jnp.int32),
            pltpu.VMEM((1, pts), jnp.int32),
            pltpu.SMEM((1, pts), jnp.int32),
            pltpu.SemaphoreType.DMA, pltpu.SemaphoreType.DMA, pltpu.SemaphoreType.DMA, pltpu.SemaphoreType.DMA,
            pltpu.SemaphoreType.DMA, pltpu.SemaphoreType.DMA((groups,)),
            pltpu.SemaphoreType.DMA, pltpu.SemaphoreType.DMA((groups,)),
            pltpu.SemaphoreType.DMA, pltpu.SemaphoreType.DMA((groups,)),
        ],
        compiler_params=pltpu.CompilerParams(collective_id=0, has_side_effects=True),
    )(owners.reshape(1, blocks), points, corner_shift, old_fields)
    return out.transpose(1, 0, 2).reshape(nvar, blocks * pts)


def solution(mesh):
    sizes = tuple(mesh.shape[a] for a in AXES)
    in_specs = (
        P(("groups", "block", "seg", "sub"), None, None),
        P(None, ("groups", "block", "seg", "sub")),
        P(None, ("groups", "block", "seg", "sub")),
        P(("groups", "block", "seg", "sub")),
    )
    out_specs = P(None, ("groups", "block", "seg", "sub"))
    return jax.shard_map(functools.partial(shards, sizes), mesh=mesh, in_specs=in_specs,
                         out_specs=out_specs, check_vma=False)
```

```python
import functools

import jax
import jax.numpy as jnp
from jax import lax
from jax.experimental import pallas as pl
from jax.experimental.pallas import tpu as pltpu
from jax.sharding import PartitionSpec as P

NEWTON = 3
CAP = 2
GROUP_PEERS = 8
AXES = ("block", "seg", "sub")

GLL_POINTS = (
    -1.0,
    -0.8717401485096066,
    -0.5917001814331423,
    -0.2092992179024789,
    0.2092992179024789,
    0.5917001814331423,
    0.8717401485096066,
    1.0,
)
WEIGHTS = []
for _n in range(8):
    _w = 1.0
    for _m in range(8):
        if _m != _n:
            _w /= GLL_POINTS[_n] - GLL_POINTS[_m]
    WEIGHTS.append(_w)

F32 = jnp.float32
BF16 = jnp.bfloat16
EXACT = lax.Precision.HIGHEST
NT = (((1,), (1,)), ((), ()))


def iota(shape, dim):
    return lax.broadcasted_iota(jnp.int32, shape, dim)


def flip(index, static):
    bit = 1
    while bit <= static:
        if static & bit:
            index = index + bit * (1 - 2 * ((index // bit) % 2))
        bit *= 2
    return index


def newton(coef, y):
    def update(xi, jac, misfit):
        m = jac
        cof = [
            [m[1][1] * m[2][2] - m[1][2] * m[2][1], m[1][2] * m[2][0] - m[1][0] * m[2][2], m[1][0] * m[2][1] - m[1][1] * m[2][0]],
            [m[0][2] * m[2][1] - m[0][1] * m[2][2], m[0][0] * m[2][2] - m[0][2] * m[2][0], m[0][1] * m[2][0] - m[0][0] * m[2][1]],
            [m[0][1] * m[1][2] - m[0][2] * m[1][1], m[0][2] * m[1][0] - m[0][0] * m[1][2], m[0][0] * m[1][1] - m[0][1] * m[1][0]],
        ]
        inv = 1.0 / (m[0][0] * cof[0][0] + m[0][1] * cof[0][1] + m[0][2] * cof[0][2])
        out = []
        for b in range(3):
            step = (cof[0][b] * misfit[0] + cof[1][b] * misfit[1] + cof[2][b] * misfit[2]) * inv
            new = -step if xi is None else xi[b] - step
            out.append(jnp.clip(new, -1.2, 1.2))
        return out

    xi = update(None, [[c[4], c[2], c[1]] for c in coef], [c[0] - t for c, t in zip(coef, y)])
    for _ in range(NEWTON - 1):
        u, v, w = xi
        uv, uw, vw = u * v, u * w, v * w
        jac, misfit = [], []
        for c, t in zip(coef, y):
            du = c[4] + c[6] * v + c[5] * w + c[7] * vw
            dv = c[2] + c[6] * u + c[3] * w + c[7] * uw
            dw = c[1] + c[5] * u + c[3] * v + c[7] * uv
            jac.append([du, dv, dw])
            misfit.append((c[0] - t) + u * du + v * (c[2] + c[3] * w) + w * c[1])
        xi = update(xi, jac, misfit)
    return xi


def lagrange(x):
    diff = [x - t for t in GLL_POINTS]
    pre = [None, diff[0]]
    for n in range(2, 8):
        pre.append(pre[-1] * diff[n - 1])
    suf = [None] * 8
    suf[6] = diff[7]
    for n in range(5, -1, -1):
        suf[n] = suf[n + 1] * diff[n + 1]
    out = []
    for n in range(8):
        value = suf[n] if n == 0 else pre[n] if n == 7 else pre[n] * suf[n]
        out.append(value * WEIGHTS[n])
    return out


def kernel(sizes, group_peers, owners_hbm, targets_hbm, shift_hbm, fields_hbm, out_ref,
           owners_ref, targets_ref, shift_ref, fbuf, table, send, recv, res, ret, lag, idsend, idrecv, ids, slotv, slots,
           osem, tsem, csem, fsem, idsem, slotsem, s0, r0, s1, r1, s2, r2):
    nb, ns, nc = sizes
    n = nb * ns * nc
    blocks = owners_ref.shape[1]
    elems = shift_ref.shape[1]
    pts = out_ref.shape[2]
    groups = n // group_peers
    lanes = idsend.shape[1]
    wide = idsend.shape[0]
    here = [lax.axis_index(a) for a in AXES]
    me = (here[0] * ns + here[1]) * nc + here[2]

    def peer(k):
        if isinstance(k, int):
            return {
                "block": flip(here[0], k // (ns * nc)),
                "seg": flip(here[1], (k // nc) % ns),
                "sub": flip(here[2], k % nc),
            }
        other = jnp.bitwise_xor(me, k)
        return {"block": other // (ns * nc), "seg": (other // nc) % ns, "sub": other % nc}

    def message(k):
        return pl.ds(8 * k if isinstance(k, int) else pl.multiple_of(8 * k, 8), 3 * CAP)

    def for_wait(first, count, ref, sem):
        part = ref.at[pl.ds(8 * first, 3 * CAP * count), :]
        pltpu.make_async_copy(part, part, sem).wait()

    def send_result(k, g):
        part = pl.ds(CAP * k, CAP)
        return pltpu.make_async_remote_copy(
            src_ref=res.at[part], dst_ref=ret.at[part], send_sem=s2, recv_sem=r2.at[g],
            device_id=peer(k), device_id_type=pl.DeviceIdType.MESH)

    get_owners = pltpu.make_async_copy(owners_hbm, owners_ref, osem)
    get_owners.start()
    get_targets = pltpu.make_async_copy(targets_hbm, targets_ref, tsem)
    get_targets.start()
    get_shift = pltpu.make_async_copy(shift_hbm, shift_ref, csem)
    get_shift.start()
    fetch = pltpu.make_async_copy(fields_hbm, fbuf, fsem)
    fetch.start()
    barrier = pltpu.get_barrier_semaphore()
    unrolled = n <= 32

    def for_peers(first, last, body):
        if unrolled:
            for k in reversed(range(first, last)):
                body(k)
        else:
            lax.fori_loop(first, last, lambda k, c: (body(k), c)[1], 0)

    for_peers(1, n, lambda k: pl.semaphore_signal(
        barrier, inc=1, device_id=peer(k), device_id_type=pl.DeviceIdType.MESH))

    shift_bits = elems.bit_length() - 1
    get_owners.wait()
    own = owners_ref[...]
    owner_dev = jnp.right_shift(own, shift_bits)
    hit = (jnp.bitwise_xor(iota((n, blocks), 0), me) == owner_dev).astype(F32)
    earlier = (iota((blocks, blocks), 0) < iota((blocks, blocks), 1)).astype(F32)
    rank = jnp.dot(hit, earlier, preferred_element_type=F32)
    match = [jnp.where(rank == float(c), hit, 0.0) for c in range(CAP)]
    both = jnp.concatenate(match, axis=0)
    get_targets.wait()
    cat = jnp.concatenate([targets_ref[:, a, :] for a in range(3)], axis=1)
    packed = jnp.dot(both, cat, precision=EXACT, preferred_element_type=F32)
    for c in range(CAP):
        part = slice(c * n, (c + 1) * n)
        for a in range(3):
            send[pl.ds(3 * c + a, n, stride=8), :] = packed[part, a * pts:(a + 1) * pts]
            recv[3 * c + a:3 * c + a + 1, :] = packed[c * n:c * n + 1, a * pts:(a + 1) * pts]
    square = (blocks, blocks)
    diag = iota(square, 0) == iota(square, 1)
    own_rows = jnp.broadcast_to(own, square)
    own_col = jnp.sum(jnp.where(diag, own_rows, 0), axis=1, keepdims=True)
    dev_col = jnp.right_shift(own_col, shift_bits)
    dev_row = jnp.right_shift(own_rows, shift_bits)
    same = jnp.where(dev_col == dev_row, 1, 0)
    rank_row = jnp.sum(jnp.where(iota(square, 0) < iota(square, 1), same, 0), axis=0, keepdims=True)
    rank_col = jnp.sum(jnp.where(iota(square, 1) < iota(square, 0), same, 0), axis=1, keepdims=True)
    place = jnp.minimum(CAP * jnp.bitwise_xor(owner_dev, me) + rank_row, CAP * n - 1)
    place = jnp.concatenate([place, jnp.zeros((1, pts - blocks), jnp.int32)], axis=1)
    elem_col = own_col - dev_col * elems
    lane_of = jnp.where(rank_col < CAP, jnp.bitwise_xor(dev_col, me) + n * rank_col, -1)
    for r in range(wide):
        here_lane = iota((blocks, lanes), 1) + lanes * r == lane_of
        row = jnp.sum(jnp.where(here_lane, elem_col, 0), axis=0, keepdims=True)
        idsend[r:r + 1, :] = row
        idrecv[r:r + 1, :] = row
    slotv[...] = place
    slot_copy = pltpu.make_async_copy(slotv, slots, slotsem)
    slot_copy.start()

    pl.semaphore_wait(barrier, n - 1)
    def send_points(k):
        g = k // group_peers
        pltpu.make_async_remote_copy(
            src_ref=idsend, dst_ref=idrecv.at[pl.ds(wide * k, wide), :], send_sem=s0, recv_sem=r0.at[g],
            device_id=peer(k), device_id_type=pl.DeviceIdType.MESH).start()
        pltpu.make_async_remote_copy(
            src_ref=send.at[message(k), :], dst_ref=recv.at[message(k), :], send_sem=s1, recv_sem=r1.at[g],
            device_id=peer(k), device_id_type=pl.DeviceIdType.MESH).start()

    for_peers(1, n, send_points)

    row, col = iota((24, 24), 0), iota((24, 24), 1)
    both_bits = jnp.bitwise_and(row, col) % 8
    odd = (both_bits + both_bits // 2 + both_bits // 4) % 2
    hada = jnp.where(row // 8 == col // 8, (1 - 2 * odd).astype(F32) * 0.125, 0.0)
    get_shift.wait()
    bits = row % 8
    sign = (1 - 2 * ((bits + bits // 2 + bits // 4) % 2)).astype(F32)
    coefs = jnp.dot(hada * sign, shift_ref[...], precision=EXACT, preferred_element_type=F32)
    c_hi = coefs.astype(BF16)
    rest = coefs - c_hi.astype(F32)
    c_mid = rest.astype(BF16)
    c_lo = (rest - c_mid.astype(F32)).astype(BF16)

    fetch.wait()
    low_sub = iota((8, 128), 0) < 4
    low_lane = iota((8, 128), 1) < 64
    keep = low_sub == low_lane

    def split(e, carry):
        parts = []
        for q in range(4):
            x = fbuf[e, :, q * 128:(q + 1) * 128]
            x = jnp.concatenate([x, x], axis=0)
            hi = x.astype(BF16).astype(F32)
            lo = x - hi
            a = jnp.where(low_sub, hi, lo)
            b = pltpu.roll(jnp.where(low_sub, lo, hi), 64, axis=1)
            parts.append(jnp.where(keep, a, b))
        table[e] = jnp.concatenate(parts, axis=0).astype(BF16)
        return carry

    lax.fori_loop(0, elems, split, 0, unroll=4)

    per = group_peers
    count = CAP * per

    def run_group(g, first):
        base = g * per
        got = per - 1 if first else per
        start = base + 1 if first else base
        for_wait(start, got, recv, r1.at[g])

        def gather(a):
            return jnp.concatenate(
                [recv[pl.ds(8 * base + 3 * c + a, per, stride=8), :] for c in range(CAP)], axis=0)

        y = [gather(a) for a in range(3)]
        taken = idrecv.at[pl.ds(wide * start, wide * got), :]
        pltpu.make_async_copy(taken, taken, r0.at[g]).wait()
        id_copy = pltpu.make_async_copy(idrecv.at[pl.ds(wide * base, wide * per), :], ids.at[pl.ds(wide * base, wide * per), :], idsem)
        id_copy.start()
        id_lane = iota((per, lanes), 1) - iota((per, lanes), 0)
        id_cols = []
        for c in range(CAP):
            at = c * n + base
            id_rows = idrecv[pl.ds(wide * base + at // lanes, per, stride=wide), :]
            id_cols.append(jnp.sum(jnp.where(id_lane == at % lanes, id_rows, 0), axis=1, keepdims=True))
        elem = jnp.concatenate(id_cols, axis=0)
        pick = jnp.where(elem == iota((count, elems), 1), 1.0, 0.0).astype(BF16)
        chosen = sum(lax.dot_general(pick, c, NT, preferred_element_type=F32) for c in (c_hi, c_mid, c_lo))
        coef = []
        for a in range(3):
            line = []
            for m in range(8):
                value = chosen[:, 8 * a + m:8 * a + m + 1]
                if m == 4 >> a:
                    value = value + 1.0
                line.append(jnp.broadcast_to(value, (count, pts)))
            coef.append(line)
        xi = newton(coef, y)
        for a in range(3):
            for i, value in enumerate(lagrange(xi[a])):
                lag[a, pl.ds(i, count, stride=8), :] = value
        id_copy.wait()
        for s in range(count):
            c, p = s // per, s % per
            e = ids[wide * (base + p) + (c * n + base) // lanes, (c * n + base) % lanes + p]
            left = table[e]
            lz = lag[2, 8 * s:8 * s + 8, :]
            w = jnp.concatenate([lag[1, 8 * s + j:8 * s + j + 1, :] * lz for j in range(8)], axis=0)
            w_hi = w.astype(BF16)
            w_lo = (w - w_hi.astype(F32)).astype(BF16)
            prod = jnp.dot(
                jnp.concatenate([left, left], axis=1),
                jnp.concatenate([w_hi, w_hi, w_lo, w_lo], axis=0),
                preferred_element_type=F32)
            total = None
            for q in range(4):
                lx = jnp.where(low_sub, lag[0, 8 * s + 2 * q:8 * s + 2 * q + 1, :],
                               lag[0, 8 * s + 2 * q + 1:8 * s + 2 * q + 2, :])
                term = prod[8 * q:8 * q + 8] * lx
                total = term if total is None else total + term
            total = total[0:4] + total[4:8]
            if first and p == 0:
                ret[c] = total
            else:
                res[CAP * (base + p) + c] = total
        for_peers_in = range(1 if first else 0, per)
        for p in for_peers_in:
            send_result(base + p, g).start()

    run_group(0, True)
    if unrolled:
        for g in range(1, groups):
            run_group(g, False)
    else:
        lax.fori_loop(1, groups, lambda g, c: (run_group(g, False), c)[1], 0)

    slot_copy.wait()
    for g in range(groups):
        start, got = (1, per - 1) if g == 0 else (g * per, per)
        back = ret.at[pl.ds(CAP * start, CAP * got)]
        pltpu.make_async_copy(back, back, r2.at[g]).wait()
    for b in range(blocks):
        out_ref[b] = ret[slots[0, b]]
    rest_ids = idrecv.at[pl.ds(wide, wide * (n - 1)), :]
    pltpu.make_async_copy(rest_ids, rest_ids, s0).wait()
    for_wait(1, n - 1, send, s1)
    left = res.at[pl.ds(CAP, CAP * (n - 1))]
    pltpu.make_async_copy(left, left, s2).wait()


def shards(sizes, old_fields, corner_shift, targets, owners):
    n = sizes[0] * sizes[1] * sizes[2]
    elems, nvar, nodes = old_fields.shape
    blocks = owners.shape[0]
    pts = targets.shape[1] // blocks
    assert n & (n - 1) == 0 and elems & (elems - 1) == 0 and nvar == 4 and nodes == 512
    group_peers = min(GROUP_PEERS, n)
    groups = n // group_peers
    wide = (CAP * n + 127) // 128
    points = targets.reshape(3, blocks, pts).transpose(1, 0, 2)
    vmem = pl.BlockSpec(memory_space=pltpu.VMEM)
    hbm = pl.BlockSpec(memory_space=pltpu.HBM)
    message = pltpu.VMEM((8 * n, pts), F32)
    result = pltpu.VMEM((CAP * n, nvar, pts), F32)
    out = pl.pallas_call(
        functools.partial(kernel, sizes, group_peers),
        out_shape=jax.ShapeDtypeStruct((blocks, nvar, pts), F32),
        in_specs=[hbm] * 4,
        out_specs=vmem,
        scratch_shapes=[
            pltpu.VMEM((1, blocks), jnp.int32),
            pltpu.VMEM((blocks, 3, pts), F32),
            pltpu.VMEM((24, elems), F32),
            pltpu.VMEM((elems, nvar, nodes), F32),
            pltpu.VMEM((elems, 32, 128), BF16),
            message, message, result, result,
            pltpu.VMEM((3, 8 * CAP * group_peers, pts), F32),
            pltpu.VMEM((wide, 128), jnp.int32),
            pltpu.VMEM((wide * n, 128), jnp.int32),
            pltpu.SMEM((wide * n, 128), jnp.int32),
            pltpu.VMEM((1, pts), jnp.int32),
            pltpu.SMEM((1, pts), jnp.int32),
            *[pltpu.SemaphoreType.DMA] * 6,
            pltpu.SemaphoreType.DMA, pltpu.SemaphoreType.DMA((groups,)),
            pltpu.SemaphoreType.DMA, pltpu.SemaphoreType.DMA((groups,)),
            pltpu.SemaphoreType.DMA, pltpu.SemaphoreType.DMA((groups,)),
        ],
        compiler_params=pltpu.CompilerParams(
            collective_id=0, has_side_effects=True, vmem_limit_bytes=16 * 1024 * 1024),
    )(*[pltpu.with_memory_space_constraint(x, pltpu.HBM) for x in (owners.reshape(1, blocks), points, corner_shift, old_fields)])
    return out.transpose(1, 0, 2).reshape(nvar, blocks * pts)


def solution(mesh):
    sizes = tuple(mesh.shape[a] for a in AXES)
    in_specs = (
        P(("groups", "block", "seg", "sub"), None, None),
        P(None, ("groups", "block", "seg", "sub")),
        P(None, ("groups", "block", "seg", "sub")),
        P(("groups", "block", "seg", "sub")),
    )
    out_specs = P(None, ("groups", "block", "seg", "sub"))
    return jax.shard_map(functools.partial(shards, sizes), mesh=mesh, in_specs=in_specs,
                         out_specs=out_specs, check_vma=False)
```

```python
import functools

import jax
import jax.numpy as jnp
from jax import lax
from jax.experimental import pallas as pl
from jax.experimental.pallas import tpu as pltpu
from jax.sharding import PartitionSpec as P

NEWTON = 3
CAP = 2
GROUP_PEERS = 4
AXES = ("block", "seg", "sub")

GLL_POINTS = (
    -1.0,
    -0.8717401485096066,
    -0.5917001814331423,
    -0.2092992179024789,
    0.2092992179024789,
    0.5917001814331423,
    0.8717401485096066,
    1.0,
)
WEIGHTS = []
for _n in range(8):
    _w = 1.0
    for _m in range(8):
        if _m != _n:
            _w /= GLL_POINTS[_n] - GLL_POINTS[_m]
    WEIGHTS.append(_w)

F32 = jnp.float32
BF16 = jnp.bfloat16
EXACT = lax.Precision.HIGHEST
NT = (((1,), (1,)), ((), ()))


def iota(shape, dim):
    return lax.broadcasted_iota(jnp.int32, shape, dim)


def flip(index, static):
    bit = 1
    while bit <= static:
        if static & bit:
            index = index + bit * (1 - 2 * ((index // bit) % 2))
        bit *= 2
    return index


def newton(coef, y):
    def update(xi, jac, misfit):
        m = jac
        cof = [
            [m[1][1] * m[2][2] - m[1][2] * m[2][1], m[1][2] * m[2][0] - m[1][0] * m[2][2], m[1][0] * m[2][1] - m[1][1] * m[2][0]],
            [m[0][2] * m[2][1] - m[0][1] * m[2][2], m[0][0] * m[2][2] - m[0][2] * m[2][0], m[0][1] * m[2][0] - m[0][0] * m[2][1]],
            [m[0][1] * m[1][2] - m[0][2] * m[1][1], m[0][2] * m[1][0] - m[0][0] * m[1][2], m[0][0] * m[1][1] - m[0][1] * m[1][0]],
        ]
        inv = 1.0 / (m[0][0] * cof[0][0] + m[0][1] * cof[0][1] + m[0][2] * cof[0][2])
        out = []
        for b in range(3):
            step = (cof[0][b] * misfit[0] + cof[1][b] * misfit[1] + cof[2][b] * misfit[2]) * inv
            new = -step if xi is None else xi[b] - step
            out.append(jnp.clip(new, -1.2, 1.2))
        return out

    xi = update(None, [[c[4], c[2], c[1]] for c in coef], [c[0] - t for c, t in zip(coef, y)])
    for _ in range(NEWTON - 1):
        u, v, w = xi
        uv, uw, vw = u * v, u * w, v * w
        jac, misfit = [], []
        for c, t in zip(coef, y):
            du = c[4] + c[6] * v + c[5] * w + c[7] * vw
            dv = c[2] + c[6] * u + c[3] * w + c[7] * uw
            dw = c[1] + c[5] * u + c[3] * v + c[7] * uv
            jac.append([du, dv, dw])
            misfit.append((c[0] - t) + u * du + v * (c[2] + c[3] * w) + w * c[1])
        xi = update(xi, jac, misfit)
    return xi


def lagrange(x):
    diff = [x - t for t in GLL_POINTS]
    pre = [None, diff[0]]
    for n in range(2, 8):
        pre.append(pre[-1] * diff[n - 1])
    suf = [None] * 8
    suf[6] = diff[7]
    for n in range(5, -1, -1):
        suf[n] = suf[n + 1] * diff[n + 1]
    out = []
    for n in range(8):
        value = suf[n] if n == 0 else pre[n] if n == 7 else pre[n] * suf[n]
        out.append(value * WEIGHTS[n])
    return out


def kernel(sizes, group_peers, owners_hbm, targets_hbm, shift_hbm, fields_hbm, out_ref,
           owners_ref, targets_ref, shift_ref, fbuf, table, send, recv, res, ret, lag, idsend, idrecv, ids, slotv, slots,
           osem, tsem, csem, fsem, idsem, slotsem, s0, r0, s1, r1, s2, r2):
    nb, ns, nc = sizes
    n = nb * ns * nc
    blocks = owners_ref.shape[1]
    elems = shift_ref.shape[1]
    pts = out_ref.shape[2]
    groups = n // group_peers
    lanes = idsend.shape[1]
    wide = idsend.shape[0]
    here = [lax.axis_index(a) for a in AXES]
    me = (here[0] * ns + here[1]) * nc + here[2]

    def peer(k):
        if isinstance(k, int):
            return {
                "block": flip(here[0], k // (ns * nc)),
                "seg": flip(here[1], (k // nc) % ns),
                "sub": flip(here[2], k % nc),
            }
        other = jnp.bitwise_xor(me, k)
        return {"block": other // (ns * nc), "seg": (other // nc) % ns, "sub": other % nc}

    def message(k):
        return pl.ds(8 * k if isinstance(k, int) else pl.multiple_of(8 * k, 8), 3 * CAP)

    def for_wait(first, count, ref, sem):
        part = ref.at[pl.ds(8 * first, 3 * CAP * count), :]
        pltpu.make_async_copy(part, part, sem).wait()

    def send_result(k, g):
        part = pl.ds(CAP * k, CAP)
        return pltpu.make_async_remote_copy(
            src_ref=res.at[part], dst_ref=ret.at[part], send_sem=s2, recv_sem=r2.at[g],
            device_id=peer(k), device_id_type=pl.DeviceIdType.MESH)

    get_owners = pltpu.make_async_copy(owners_hbm, owners_ref, osem)
    get_owners.start()
    get_targets = pltpu.make_async_copy(targets_hbm, targets_ref, tsem)
    get_targets.start()
    get_shift = pltpu.make_async_copy(shift_hbm, shift_ref, csem)
    get_shift.start()
    fetch = pltpu.make_async_copy(fields_hbm, fbuf, fsem)
    fetch.start()
    barrier = pltpu.get_barrier_semaphore()
    unrolled = n <= 32

    def for_peers(first, last, body):
        if unrolled:
            for k in reversed(range(first, last)):
                body(k)
        else:
            lax.fori_loop(first, last, lambda k, c: (body(k), c)[1], 0)

    for_peers(1, n, lambda k: pl.semaphore_signal(
        barrier, inc=1, device_id=peer(k), device_id_type=pl.DeviceIdType.MESH))

    shift_bits = elems.bit_length() - 1
    get_owners.wait()
    own = owners_ref[...]
    owner_dev = jnp.right_shift(own, shift_bits)
    hit = (jnp.bitwise_xor(iota((n, blocks), 0), me) == owner_dev).astype(F32)
    earlier = (iota((blocks, blocks), 0) < iota((blocks, blocks), 1)).astype(F32)
    rank = jnp.dot(hit, earlier, preferred_element_type=F32)
    match = [jnp.where(rank == float(c), hit, 0.0) for c in range(CAP)]
    both = jnp.concatenate(match, axis=0)
    get_targets.wait()
    cat = jnp.concatenate([targets_ref[:, a, :] for a in range(3)], axis=1)
    packed = jnp.dot(both, cat, precision=EXACT, preferred_element_type=F32)
    for c in range(CAP):
        part = slice(c * n, (c + 1) * n)
        for a in range(3):
            send[pl.ds(3 * c + a, n, stride=8), :] = packed[part, a * pts:(a + 1) * pts]
            recv[3 * c + a:3 * c + a + 1, :] = packed[c * n:c * n + 1, a * pts:(a + 1) * pts]
    square = (blocks, blocks)
    diag = iota(square, 0) == iota(square, 1)
    own_rows = jnp.broadcast_to(own, square)
    own_col = jnp.sum(jnp.where(diag, own_rows, 0), axis=1, keepdims=True)
    dev_col = jnp.right_shift(own_col, shift_bits)
    dev_row = jnp.right_shift(own_rows, shift_bits)
    same = jnp.where(dev_col == dev_row, 1, 0)
    rank_row = jnp.sum(jnp.where(iota(square, 0) < iota(square, 1), same, 0), axis=0, keepdims=True)
    rank_col = jnp.sum(jnp.where(iota(square, 1) < iota(square, 0), same, 0), axis=1, keepdims=True)
    place = jnp.minimum(CAP * jnp.bitwise_xor(owner_dev, me) + rank_row, CAP * n - 1)
    place = jnp.concatenate([place, jnp.zeros((1, pts - blocks), jnp.int32)], axis=1)
    elem_col = own_col - dev_col * elems
    lane_of = jnp.where(rank_col < CAP, jnp.bitwise_xor(dev_col, me) + n * rank_col, -1)
    for r in range(wide):
        here_lane = iota((blocks, lanes), 1) + lanes * r == lane_of
        row = jnp.sum(jnp.where(here_lane, elem_col, 0), axis=0, keepdims=True)
        idsend[r:r + 1, :] = row
        idrecv[r:r + 1, :] = row
    slotv[...] = place
    slot_copy = pltpu.make_async_copy(slotv, slots, slotsem)
    slot_copy.start()

    pl.semaphore_wait(barrier, n - 1)
    def send_points(k):
        g = k // group_peers
        pltpu.make_async_remote_copy(
            src_ref=idsend, dst_ref=idrecv.at[pl.ds(wide * k, wide), :], send_sem=s0, recv_sem=r0.at[g],
            device_id=peer(k), device_id_type=pl.DeviceIdType.MESH).start()
        pltpu.make_async_remote_copy(
            src_ref=send.at[message(k), :], dst_ref=recv.at[message(k), :], send_sem=s1, recv_sem=r1.at[g],
            device_id=peer(k), device_id_type=pl.DeviceIdType.MESH).start()

    for_peers(1, n, send_points)

    row, col = iota((24, 24), 0), iota((24, 24), 1)
    both_bits = jnp.bitwise_and(row, col) % 8
    odd = (both_bits + both_bits // 2 + both_bits // 4) % 2
    hada = jnp.where(row // 8 == col // 8, (1 - 2 * odd).astype(F32) * 0.125, 0.0)
    get_shift.wait()
    bits = row % 8
    sign = (1 - 2 * ((bits + bits // 2 + bits // 4) % 2)).astype(F32)
    coefs = jnp.dot(hada * sign, shift_ref[...], precision=EXACT, preferred_element_type=F32)
    c_hi = coefs.astype(BF16)
    rest = coefs - c_hi.astype(F32)
    c_mid = rest.astype(BF16)
    c_lo = (rest - c_mid.astype(F32)).astype(BF16)

    fetch.wait()
    low_sub = iota((8, 128), 0) < 4
    low_lane = iota((8, 128), 1) < 64
    keep = low_sub == low_lane

    def split(e, carry):
        parts = []
        for q in range(4):
            x = fbuf[e, :, q * 128:(q + 1) * 128]
            x = jnp.concatenate([x, x], axis=0)
            hi = x.astype(BF16).astype(F32)
            lo = x - hi
            a = jnp.where(low_sub, hi, lo)
            b = pltpu.roll(jnp.where(low_sub, lo, hi), 64, axis=1)
            parts.append(jnp.where(keep, a, b))
        table[e] = jnp.concatenate(parts, axis=0).astype(BF16)
        return carry

    lax.fori_loop(0, elems, split, 0, unroll=4)

    per = group_peers
    count = CAP * per

    def run_group(g, first):
        base = g * per
        got = per - 1 if first else per
        start = base + 1 if first else base
        for_wait(start, got, recv, r1.at[g])

        def gather(a):
            return jnp.concatenate(
                [recv[pl.ds(8 * base + 3 * c + a, per, stride=8), :] for c in range(CAP)], axis=0)

        y = [gather(a) for a in range(3)]
        taken = idrecv.at[pl.ds(wide * start, wide * got), :]
        pltpu.make_async_copy(taken, taken, r0.at[g]).wait()
        id_copy = pltpu.make_async_copy(idrecv.at[pl.ds(wide * base, wide * per), :], ids.at[pl.ds(wide * base, wide * per), :], idsem)
        id_copy.start()
        id_lane = iota((per, lanes), 1) - iota((per, lanes), 0)
        id_cols = []
        for c in range(CAP):
            at = c * n + base
            id_rows = idrecv[pl.ds(wide * base + at // lanes, per, stride=wide), :]
            id_cols.append(jnp.sum(jnp.where(id_lane == at % lanes, id_rows, 0), axis=1, keepdims=True))
        elem = jnp.concatenate(id_cols, axis=0)
        pick = jnp.where(elem == iota((count, elems), 1), 1.0, 0.0).astype(BF16)
        chosen = sum(lax.dot_general(pick, c, NT, preferred_element_type=F32) for c in (c_hi, c_mid, c_lo))
        coef = []
        for a in range(3):
            line = []
            for m in range(8):
                value = chosen[:, 8 * a + m:8 * a + m + 1]
                if m == 4 >> a:
                    value = value + 1.0
                line.append(jnp.broadcast_to(value, (count, pts)))
            coef.append(line)
        xi = newton(coef, y)
        for a in range(3):
            for i, value in enumerate(lagrange(xi[a])):
                lag[a, pl.ds(i, count, stride=8), :] = value
        id_copy.wait()
        for s in range(count):
            c, p = s // per, s % per
            e = ids[wide * (base + p) + (c * n + base) // lanes, (c * n + base) % lanes + p]
            left = table[e]
            lz = lag[2, 8 * s:8 * s + 8, :]
            w = jnp.concatenate([lag[1, 8 * s + j:8 * s + j + 1, :] * lz for j in range(8)], axis=0)
            w_hi = w.astype(BF16)
            w_lo = (w - w_hi.astype(F32)).astype(BF16)
            prod = jnp.dot(
                jnp.concatenate([left, left], axis=1),
                jnp.concatenate([w_hi, w_hi, w_lo, w_lo], axis=0),
                preferred_element_type=F32)
            total = None
            for q in range(4):
                lx = jnp.where(low_sub, lag[0, 8 * s + 2 * q:8 * s + 2 * q + 1, :],
                               lag[0, 8 * s + 2 * q + 1:8 * s + 2 * q + 2, :])
                term = prod[8 * q:8 * q + 8] * lx
                total = term if total is None else total + term
            total = total[0:4] + total[4:8]
            if first and p == 0:
                ret[c] = total
            else:
                res[CAP * (base + p) + c] = total
        for_peers_in = range(1 if first else 0, per)
        for p in for_peers_in:
            send_result(base + p, g).start()

    run_group(0, True)
    if unrolled:
        for g in range(1, groups):
            run_group(g, False)
    else:
        lax.fori_loop(1, groups, lambda g, c: (run_group(g, False), c)[1], 0)

    slot_copy.wait()
    for g in range(groups):
        start, got = (1, per - 1) if g == 0 else (g * per, per)
        back = ret.at[pl.ds(CAP * start, CAP * got)]
        pltpu.make_async_copy(back, back, r2.at[g]).wait()
    for b in range(blocks):
        out_ref[b] = ret[slots[0, b]]
    rest_ids = idrecv.at[pl.ds(wide, wide * (n - 1)), :]
    pltpu.make_async_copy(rest_ids, rest_ids, s0).wait()
    for_wait(1, n - 1, send, s1)
    left = res.at[pl.ds(CAP, CAP * (n - 1))]
    pltpu.make_async_copy(left, left, s2).wait()


def shards(sizes, old_fields, corner_shift, targets, owners):
    n = sizes[0] * sizes[1] * sizes[2]
    elems, nvar, nodes = old_fields.shape
    blocks = owners.shape[0]
    pts = targets.shape[1] // blocks
    assert n & (n - 1) == 0 and elems & (elems - 1) == 0 and nvar == 4 and nodes == 512
    group_peers = min(GROUP_PEERS, n)
    groups = n // group_peers
    wide = (CAP * n + 127) // 128
    points = targets.reshape(3, blocks, pts).transpose(1, 0, 2)
    vmem = pl.BlockSpec(memory_space=pltpu.VMEM)
    hbm = pl.BlockSpec(memory_space=pltpu.HBM)
    message = pltpu.VMEM((8 * n, pts), F32)
    result = pltpu.VMEM((CAP * n, nvar, pts), F32)
    out = pl.pallas_call(
        functools.partial(kernel, sizes, group_peers),
        out_shape=jax.ShapeDtypeStruct((blocks, nvar, pts), F32),
        in_specs=[hbm] * 4,
        out_specs=vmem,
        scratch_shapes=[
            pltpu.VMEM((1, blocks), jnp.int32),
            pltpu.VMEM((blocks, 3, pts), F32),
            pltpu.VMEM((24, elems), F32),
            pltpu.VMEM((elems, nvar, nodes), F32),
            pltpu.VMEM((elems, 32, 128), BF16),
            message, message, result, result,
            pltpu.VMEM((3, 8 * CAP * group_peers, pts), F32),
            pltpu.VMEM((wide, 128), jnp.int32),
            pltpu.VMEM((wide * n, 128), jnp.int32),
            pltpu.SMEM((wide * n, 128), jnp.int32),
            pltpu.VMEM((1, pts), jnp.int32),
            pltpu.SMEM((1, pts), jnp.int32),
            *[pltpu.SemaphoreType.DMA] * 6,
            pltpu.SemaphoreType.DMA, pltpu.SemaphoreType.DMA((groups,)),
            pltpu.SemaphoreType.DMA, pltpu.SemaphoreType.DMA((groups,)),
            pltpu.SemaphoreType.DMA, pltpu.SemaphoreType.DMA((groups,)),
        ],
        compiler_params=pltpu.CompilerParams(
            collective_id=0, has_side_effects=True, vmem_limit_bytes=16 * 1024 * 1024),
    )(*[pltpu.with_memory_space_constraint(x, pltpu.HBM) for x in (owners.reshape(1, blocks), points, corner_shift, old_fields)])
    return out.transpose(1, 0, 2).reshape(nvar, blocks * pts)


def solution(mesh):
    sizes = tuple(mesh.shape[a] for a in AXES)
    in_specs = (
        P(("groups", "block", "seg", "sub"), None, None),
        P(None, ("groups", "block", "seg", "sub")),
        P(None, ("groups", "block", "seg", "sub")),
        P(("groups", "block", "seg", "sub")),
    )
    out_specs = P(None, ("groups", "block", "seg", "sub"))
    return jax.shard_map(functools.partial(shards, sizes), mesh=mesh, in_specs=in_specs,
                         out_specs=out_specs, check_vma=False)
```
